32 devices in a mesh: gx: 4 (over z), gy: 2 (over y), gz: 4 (over x, core).
Axes of the slice: x: 2, y: 2, z: 4, core: 2. Of those that a mesh axis runs over, the one named last changes fastest.
Arguments:
- displacement: float32 [3, 64, 64, 1024], P(None, 'gx', 'gy', 'gz'), may hold values from -1.5 to 1.5
- density: float32 [64, 64, 1024], P('gx', 'gy', 'gz'), may hold values from 0.03 to 1
- stiffness: float32 [24, 24], replicated, may hold values from -9 to 9.5, as said below
Outputs:
- filtered: float32 [64, 64, 1024], P('gx', 'gy', 'gz')
- compliance: float32 [], replicated
- volume: float32 [], replicated
The draws below stay inside these ranges and needn't reach their ends.
Inputs may be any that keep to these rules, and one draw needn't show every extreme that they name: `stiffness`: symmetric and positive definite, every eigenvalue at least 0.5.
All inputs are finite; a program needn't handle non-finite values.
Results may differ from the reference program's by a relative error of at most 0.00005.
Values sent between devices are 32-bit elements; how exact they have to be, the bound alone decides.
No kernel may reach another device: no remote copies, remote signals or barrier semaphores. Data moves between devices by JAX's collectives and lax.ppermute only.
A program may use at most 64 MiB of HBM per device.

```python
import jax
import jax.numpy as jnp
from jax import lax

NX = 64
NY = 64
NZ = 1024


def draw_density(key, part):
    levels = jax.random.uniform(key, (NX, NY, NZ), jnp.float32, 0.1, 1.0)
    rising = (1.0 + 2.0 * jnp.arange(NX, dtype=jnp.float32) / max(NX - 1, 1)) / 3.0
    return levels * rising[:, None, None]


def draw_stiffness(key, part):
    factors = jax.random.truncated_normal(key, -3.0, 3.0, (24, 24), jnp.float32)
    factors = factors / jnp.sqrt(24.0)
    return jnp.dot(factors, factors.T, precision=lax.Precision.HIGHEST) + 0.5 * jnp.eye(24, dtype=jnp.float32)


def level_of(own_key, dims, cuts, least, top_value):
    def one(axis_at, shards_of):
        steps = jax.random.uniform(jax.random.fold_in(jax.random.fold_in(own_key, 6), axis_at), (shards_of,), jnp.float32, least / len(cuts), top_value / len(cuts))
        return jnp.repeat(jnp.exp(steps), dims[axis_at] // shards_of).reshape((-1,) + (1,) * (len(dims) - axis_at - 1))

    level = one(*cuts[0])
    for cut in cuts[1:]:
        level = level * one(*cut)
    return level


def bell_draw(key, dims, deviation, bound, pieces=(), kind=jnp.bfloat16):
    values = deviation * jax.random.normal(key, dims, jnp.float32)
    if pieces:
        values = values * level_of(key, dims, pieces, -0.22, 0.18)
    return jnp.clip(values, -bound, bound).astype(kind)


def setup_inputs(seed: int = 0) -> dict:
    seeds = jax.random.split(jax.random.key(seed), 4)
    displacement = bell_draw(seeds[0], (3, NX, NY, NZ), 0.25, 1.5, ((1, 4), (2, 2), (3, 4)), jnp.float32)
    density = draw_density(jax.random.fold_in(seeds[3], 71), 0)
    stiffness = draw_stiffness(jax.random.fold_in(seeds[3], 71), 0)
    return {"displacement": displacement, "density": density, "stiffness": stiffness}


VOID_STIFFNESS = 1e-3
KERNEL = (1.0, 2.0, 3.0, 2.0, 1.0)


def smooth(values, along):
    length = values.shape[along] - 4
    summed = None
    for offset in range(5):
        section = lax.slice_in_dim(values, offset, offset + length, axis=along)
        scaled = KERNEL[offset] * section
        summed = scaled if summed is None else summed + scaled
    return summed


def side_sums(first, amount, extent):
    position = first + jnp.arange(amount, dtype=jnp.int32)
    summed = jnp.zeros((amount,), jnp.float32)
    for offset in range(5):
        inside = (position + offset - 2 >= 0) & (position + offset - 2 < extent)
        summed = summed + KERNEL[offset] * inside.astype(jnp.float32)
    return summed


def plane_energy(slab_nodes, stiffness):
    height = slab_nodes.shape[2] - 1
    length = slab_nodes.shape[3] - 1
    corner_rows = jnp.stack([slab_nodes[member, along_x, along_y:along_y + height, along_z:along_z + length].reshape(-1)
                             for member in range(3) for along_x in range(2) for along_y in range(2) for along_z in range(2)])
    product = jnp.dot(stiffness, corner_rows, precision=lax.Precision.HIGHEST, preferred_element_type=jnp.float32)
    return jnp.sum(corner_rows * product, axis=0).reshape(height, length)


def energies(node_field, stiffness, planes):
    def one_plane(plane_index):
        slab_nodes = lax.dynamic_slice_in_dim(node_field, plane_index, 2, 1)
        return plane_energy(slab_nodes, stiffness)
    return lax.map(one_plane, jnp.arange(planes, dtype=jnp.int32))


def reference(displacement, density, stiffness):
    node_field = jnp.pad(displacement, ((0, 0), (0, 1), (0, 1), (0, 1)))
    energy = energies(node_field, stiffness, NX)
    modulus = VOID_STIFFNESS + density * density * density * (1.0 - VOID_STIFFNESS)
    cell_count = float(NX * NY * NZ)
    compliance = jnp.sum(modulus * energy) / cell_count
    volume = jnp.sum(density) / cell_count
    sensitivity = -3.0 * (1.0 - VOID_STIFFNESS) * density * density * energy
    hole_sum = side_sums(0, NX, NX)[:, None, None] * side_sums(0, NY, NY)[None, :, None] * side_sums(0, NZ, NZ)[None, None, :]
    weighted = sensitivity / hole_sum
    padded = jnp.pad(weighted, 2)
    filtered = smooth(smooth(smooth(padded, 0), 1), 2)
    return filtered, compliance, volume
```

```python
import functools

import jax
import jax.numpy as jnp
from jax import lax
from jax.experimental import pallas as pl
from jax.experimental.pallas import tpu as pltpu
from jax.sharding import PartitionSpec as P

VOID = 0.001
AXES = ("gx", "gy", "gz")
F32 = jnp.float32
BF16 = jnp.bfloat16
LANES = 128
ROWS = 8


def shift_from(block, axis, distance):
    count = lax.axis_size(axis)
    route = [(i + distance, i) for i in range(count) if 0 <= i + distance < count]
    return lax.ppermute(block, axis, route)


def both_sides(low_part, high_part, axis):
    count = lax.axis_size(axis)
    if count == 2:
        at = lax.axis_index(axis)
        got = lax.ppermute(jnp.where(at == 0, high_part, low_part), axis, [(0, 1), (1, 0)])
        zero = jnp.zeros_like(got)
        return jnp.where(at == 1, got, zero), jnp.where(at == 0, got, zero)
    return shift_from(high_part, axis, -1), shift_from(low_part, axis, 1)


def missing(position, extent):
    lost = (
        3.0 * (position == 0).astype(F32)
        + 1.0 * (position == 1).astype(F32)
        + 3.0 * (position == extent - 1).astype(F32)
        + 1.0 * (position == extent - 2).astype(F32)
    )
    return 9.0 - lost


def energy_kernel(
    where_ref, u_ref, xh_ref, yh_ref, zh_ref, rho_ref, k_ref, w_ref, sums_ref, corners, gains, inv_ref,
    *, extents
):
    planes, height, length = rho_ref.shape
    side = 24 * ROWS

    k = k_ref[...]
    k_hi = k.astype(BF16)
    k_lo = (k - k_hi.astype(F32)).astype(BF16)
    r0 = lax.broadcasted_iota(jnp.int32, (side, 24), 0)
    r1 = lax.broadcasted_iota(jnp.int32, (side, 24), 1)
    spread = (r0 // ROWS == r1).astype(F32).astype(BF16)
    d0 = lax.broadcasted_iota(jnp.int32, (side, side), 0)
    d1 = lax.broadcasted_iota(jnp.int32, (side, side), 1)
    same_row = (d0 % ROWS) == (d1 % ROWS)
    for part, kk in enumerate((k_hi, k_lo)):
        tall = jnp.dot(spread, kk, preferred_element_type=F32).astype(BF16)
        full = lax.dot_general(tall, spread, (((1,), (1,)), ((), ())), preferred_element_type=F32)
        gains[part * side : (part + 1) * side, :] = jnp.where(same_row, full, 0.0).astype(BF16)

    row = lax.broadcasted_iota(jnp.int32, (height, length), 0)
    lane = lax.broadcasted_iota(jnp.int32, (height, length), 1)
    second = missing(row + where_ref[1] * height, extents[1])
    third = missing(lane + where_ref[2] * length, extents[2])
    inv_ref[...] = (-3.0 * (1.0 - VOID)) / (second * third)
    last_row = row == height - 1
    last_lane = lane == length - 1

    def prepare(plane_of, p, slot):
        turned = zh_ref[p].T
        for m in range(3):
            plane = plane_of(m)
            col0 = turned[0:height, m : m + 1]
            col1 = turned[0:height, m + 4 : m + 5]
            up = jnp.where(last_row, yh_ref[m, pl.ds(p, 1), :], pltpu.roll(plane, height - 1, 0))
            corners[slot, 4 * m + 0] = plane
            corners[slot, 4 * m + 1] = jnp.where(last_lane, col0, pltpu.roll(plane, length - 1, 1))
            corners[slot, 4 * m + 2] = up
            corners[slot, 4 * m + 3] = jnp.where(last_lane, col1, pltpu.roll(up, length - 1, 1))

    prepare(lambda m: u_ref[m, 0], 0, 0)

    def element_plane(i, slot, nxt, sums):
        total, amount = sums
        first = missing(where_ref[0] * planes + i + jnp.zeros((ROWS, length), jnp.int32), extents[0])
        inv_first = 1.0 / first
        for j in range(height // ROWS):
            rows = slice(j * ROWS, (j + 1) * ROWS)
            x = jnp.concatenate(
                [
                    corners[(slot, nxt)[a], 4 * m + 2 * b + c, rows, :]
                    for m in range(3)
                    for a in range(2)
                    for b in range(2)
                    for c in range(2)
                ],
                axis=0,
            )
            h = x.astype(BF16)
            y = jnp.dot(gains[...], h, preferred_element_type=F32)
            y = y[:side] + y[side:]
            e = ((2.0 * x - h.astype(F32)) * y).reshape(24, ROWS, length).sum(axis=0)
            rho = rho_ref[i, rows, :]
            square = rho * rho
            w_ref[i, rows, :] = square * e * (inv_ref[rows, :] * inv_first)
            total = total + (VOID + square * rho * (1.0 - VOID)) * e
            amount = amount + rho
        return total, amount

    def step(i, sums):
        slot = lax.rem(i, 2)
        prepare(lambda m: u_ref[m, i + 1], i + 1, 1 - slot)
        return element_plane(i, slot, 1 - slot, sums)

    zero = jnp.zeros((ROWS, length), F32)
    sums = lax.fori_loop(0, planes - 1, step, (zero, zero))
    slot = (planes - 1) % 2
    prepare(lambda m: xh_ref[m, 0], planes, 1 - slot)
    total, amount = element_plane(planes - 1, slot, 1 - slot, sums)
    at = lax.broadcasted_iota(jnp.int32, sums_ref.shape, 1)
    sums_ref[...] = jnp.where(at == 0, jnp.sum(total), jnp.where(at == 1, jnp.sum(amount), 0.0))


def filter_kernel(w_ref, xlo_ref, xhi_ref, ylo_ref, yhi_ref, z_ref, out_ref, field):
    planes, height, length = w_ref.shape
    full_rows, full_lanes = field.shape[1:]

    def fill(p, body):
        field[p, 0:height, 0:length] = body
        tail = jnp.concatenate(
            [yhi_ref[p], jnp.zeros((ROWS - 4, length), F32), ylo_ref[p]], axis=0
        )
        field[p, height : height + ROWS, 0:length] = tail
        z = z_ref[p]
        block = jnp.concatenate([z[0:2], jnp.zeros((LANES - 4, LANES), F32), z[2:4]], axis=0)
        field[p, :, length : length + LANES] = block.T[0:full_rows]

    def box(v, axis):
        n = v.shape[axis]
        return v + pltpu.roll(v, 1, axis) + pltpu.roll(v, n - 1, axis)

    for p in range(2):
        fill(p, xlo_ref[p])
        fill(planes + 2 + p, xhi_ref[p])

    def middle(p, carry):
        fill(p + 2, w_ref[p])
        return carry

    lax.fori_loop(0, planes, middle, 0)

    def one(i, carry):
        a, b, c, d, e = (field[i + k] for k in range(5))
        t = (a + e) + 2.0 * (b + d) + 3.0 * c
        t = box(box(t, 0), 0)[0:height]
        t = box(box(t, 1), 1)
        out_ref[i] = t[:, 0:length]
        return carry

    lax.fori_loop(0, planes, one, 0)


VMEM = pl.BlockSpec(memory_space=pltpu.VMEM)
SMEM = pl.BlockSpec(memory_space=pltpu.SMEM)


def on_device(displacement, density, stiffness):
    planes, height, length = density.shape
    sizes = tuple(lax.axis_size(a) for a in AXES)
    devices = sizes[0] * sizes[1] * sizes[2]
    extents = tuple(n * s for n, s in zip(density.shape, sizes))
    where = jnp.stack([lax.axis_index(a) for a in AXES]).astype(jnp.int32)

    xh = shift_from(displacement[:, :1], "gx", 1)
    yrow = jnp.concatenate([displacement[:, :, 0], xh[:, :, 0]], axis=1)
    yh = shift_from(yrow, "gy", 1)
    zcol = jnp.concatenate([displacement[..., 0], xh[..., 0]], axis=1)
    zcol = jnp.concatenate([zcol, yh[..., :1]], axis=2)
    zh = shift_from(zcol.transpose(1, 0, 2), "gz", 1)
    gap = LANES - height
    zh = jnp.concatenate(
        [
            jnp.pad(zh[..., :height], ((0, 0), (0, 1), (0, gap))),
            jnp.pad(zh[..., 1:], ((0, 0), (0, 1), (0, gap))),
        ],
        axis=1,
    )

    weighted, sums = pl.pallas_call(
        functools.partial(energy_kernel, extents=extents),
        in_specs=[SMEM] + [VMEM] * 6,
        out_specs=[VMEM, VMEM],
        out_shape=[
            jax.ShapeDtypeStruct(density.shape, F32),
            jax.ShapeDtypeStruct((devices, LANES), F32),
        ],
        scratch_shapes=[
            pltpu.VMEM((2, 12, height, length), F32),
            pltpu.VMEM((48 * ROWS, 24 * ROWS), BF16),
            pltpu.VMEM((height, length), F32),
        ],
        name="energy",
    )(where, displacement, xh, yh, zh, density, stiffness)

    gathered = lax.all_to_all(sums, AXES, 0, 0, tiled=True)
    totals = jnp.sum(gathered, axis=0)

    xlo, xhi = both_sides(weighted[:2], weighted[-2:], "gx")
    low = jnp.concatenate([v[:, :2] for v in (xlo, weighted, xhi)], axis=0)
    high = jnp.concatenate([v[:, -2:] for v in (xlo, weighted, xhi)], axis=0)
    ylo, yhi = both_sides(low, high, "gy")

    def columns(part):
        middle = jnp.concatenate([v[..., part] for v in (xlo, weighted, xhi)], axis=0)
        gap = jnp.zeros((planes + 4, ROWS - 4, 2), F32)
        whole = jnp.concatenate([middle, yhi[..., part], gap, ylo[..., part]], axis=1)
        return whole.transpose(0, 2, 1)

    zlo, zhi = both_sides(columns(slice(0, 2)), columns(slice(length - 2, length)), "gz")
    z = jnp.pad(jnp.concatenate([zhi, zlo], axis=1), ((0, 0), (0, 4), (0, LANES - height - ROWS)))

    filtered = pl.pallas_call(
        filter_kernel,
        in_specs=[VMEM] * 6,
        out_specs=VMEM,
        out_shape=jax.ShapeDtypeStruct(density.shape, F32),
        scratch_shapes=[pltpu.VMEM((planes + 4, height + ROWS, length + LANES), F32)],
        name="cone",
    )(weighted, xlo, xhi, ylo, yhi, z)

    cells = float(extents[0] * extents[1] * extents[2])
    return filtered, totals[0] / cells, totals[1] / cells


def solution(mesh):
    return jax.shard_map(
        on_device,
        mesh=mesh,
        in_specs=(P(None, *AXES), P(*AXES), P()),
        out_specs=(P(*AXES), P(), P()),
        check_vma=False,
    )
```

```python
import functools

import jax
import jax.numpy as jnp
from jax import lax
from jax.experimental import pallas as pl
from jax.experimental.pallas import tpu as pltpu
from jax.sharding import PartitionSpec as P

VOID = 0.001
AXES = ("gx", "gy", "gz")
F32 = jnp.float32
BF16 = jnp.bfloat16
LANES = 128
ROWS = 8


def shift_from(block, axis, distance):
    count = lax.axis_size(axis)
    route = [(i + distance, i) for i in range(count) if 0 <= i + distance < count]
    return lax.ppermute(block, axis, route)


def missing(position, extent):
    lost = (
        3.0 * (position == 0).astype(F32)
        + 1.0 * (position == 1).astype(F32)
        + 3.0 * (position == extent - 1).astype(F32)
        + 1.0 * (position == extent - 2).astype(F32)
    )
    return 9.0 - lost


def energy_kernel(
    where_ref, u_ref, xh_ref, yh_ref, zh_ref, rho_ref, k_ref,
    w_ref, low_ref, high_ref, sums_ref, corners, gains, inv_ref, *, extents
):
    planes, height, length = rho_ref.shape
    side = 24 * ROWS

    k = k_ref[...]
    k_hi = k.astype(BF16)
    k_lo = (k - k_hi.astype(F32)).astype(BF16)
    r0 = lax.broadcasted_iota(jnp.int32, (side, 24), 0)
    r1 = lax.broadcasted_iota(jnp.int32, (side, 24), 1)
    spread = (r0 // ROWS == r1).astype(F32).astype(BF16)
    d0 = lax.broadcasted_iota(jnp.int32, (side, side), 0)
    d1 = lax.broadcasted_iota(jnp.int32, (side, side), 1)
    same_row = (d0 % ROWS) == (d1 % ROWS)
    for part, kk in enumerate((k_hi, k_lo)):
        tall = jnp.dot(spread, kk, preferred_element_type=F32).astype(BF16)
        full = lax.dot_general(tall, spread, (((1,), (1,)), ((), ())), preferred_element_type=F32)
        gains[part * side : (part + 1) * side, :] = jnp.where(same_row, full, 0.0).astype(BF16)

    row = lax.broadcasted_iota(jnp.int32, (height, length), 0)
    lane = lax.broadcasted_iota(jnp.int32, (height, length), 1)
    second = missing(row + where_ref[1] * height, extents[1])
    third = missing(lane + where_ref[2] * length, extents[2])
    inv_ref[...] = (-3.0 * (1.0 - VOID)) / (second * third)
    last_row = row == height - 1
    last_lane = lane == length - 1

    def prepare(plane_of, p, slot):
        turned = zh_ref[p].T
        for m in range(3):
            plane = plane_of(m)
            col0 = turned[0:height, m : m + 1]
            col1 = turned[0:height, m + 4 : m + 5]
            up = jnp.where(last_row, yh_ref[m, pl.ds(p, 1), :], pltpu.roll(plane, height - 1, 0))
            corners[slot, 4 * m + 0] = plane
            corners[slot, 4 * m + 1] = jnp.where(last_lane, col0, pltpu.roll(plane, length - 1, 1))
            corners[slot, 4 * m + 2] = up
            corners[slot, 4 * m + 3] = jnp.where(last_lane, col1, pltpu.roll(up, length - 1, 1))

    prepare(lambda m: u_ref[m, 0], 0, 0)

    def element_plane(i, slot, nxt, sums):
        total, amount = sums
        first = missing(where_ref[0] * planes + i + jnp.zeros((ROWS, length), jnp.int32), extents[0])
        inv_first = 1.0 / first
        for j in range(height // ROWS):
            rows = slice(j * ROWS, (j + 1) * ROWS)
            x = jnp.concatenate(
                [
                    corners[(slot, nxt)[a], 4 * m + 2 * b + c, rows, :]
                    for m in range(3)
                    for a in range(2)
                    for b in range(2)
                    for c in range(2)
                ],
                axis=0,
            )
            h = x.astype(BF16)
            y = jnp.dot(gains[...], h, preferred_element_type=F32)
            y = y[:side] + y[side:]
            e = ((2.0 * x - h.astype(F32)) * y).reshape(24, ROWS, length).sum(axis=0)
            rho = rho_ref[i, rows, :]
            square = rho * rho
            w_ref[i, rows, :] = square * e * (inv_ref[rows, :] * inv_first)
            total = total + (VOID + square * rho * (1.0 - VOID)) * e
            amount = amount + rho
        return total, amount

    def step(i, sums):
        slot = lax.rem(i, 2)
        prepare(lambda m: u_ref[m, i + 1], i + 1, 1 - slot)
        return element_plane(i, slot, 1 - slot, sums)

    zero = jnp.zeros((ROWS, length), F32)
    sums = lax.fori_loop(0, planes - 1, step, (zero, zero))
    slot = (planes - 1) % 2
    prepare(lambda m: xh_ref[m, 0], planes, 1 - slot)
    total, amount = element_plane(planes - 1, slot, 1 - slot, sums)
    low_ref[...] = w_ref[0:2]
    high_ref[...] = w_ref[planes - 2 : planes]
    at = lax.broadcasted_iota(jnp.int32, sums_ref.shape, 2)
    sums_ref[...] = jnp.where(at == 0, jnp.sum(total), jnp.where(at == 1, jnp.sum(amount), 0.0))


def box(v, axis):
    n = v.shape[axis]
    return v + pltpu.roll(v, 1, axis) + pltpu.roll(v, n - 1, axis)


def first_kernel(where_ref, w_ref, xlo_ref, xhi_ref, out_ref, *messages):
    planes, height, _ = w_ref.shape

    def emit(i, five):
        a, b, c, d, e = five
        t = (a + e) + 2.0 * (b + d) + 3.0 * c
        out_ref[i] = t
        low, high = t[0:2], t[height - 2 : height]
        if len(messages) == 1:
            messages[0][i] = jnp.where(where_ref[1] == 0, high, low)
        else:
            messages[0][i] = low
            messages[1][i] = high

    def plane(k):
        if k < 0:
            return xlo_ref[2 + k]
        return w_ref[k] if k < planes else xhi_ref[k - planes]

    for i in (0, 1, planes - 2, planes - 1):
        emit(i, [plane(i + d) for d in range(-2, 3)])

    def inner(i, carry):
        emit(i, [w_ref[i + d] for d in range(-2, 3)])
        return carry

    lax.fori_loop(2, planes - 2, inner, 0, unroll=2)


def second_kernel(where_ref, s_ref, *refs):
    planes, height, length = s_ref.shape
    messages, (out_ref, low_ref, high_ref) = refs[:-3], refs[-3:]

    def one(i, carry):
        if len(messages) == 1:
            got = messages[0][i]
            before = jnp.where(where_ref[1] == 1, got, 0.0)
            after = jnp.where(where_ref[1] == 0, got, 0.0)
        else:
            before, after = messages[0][i], messages[1][i]
        gap = jnp.zeros((ROWS - 4, length), F32)
        t = jnp.concatenate([s_ref[i], after, gap, before], axis=0)
        t = box(box(t, 0), 0)[0:height]
        out_ref[i] = t
        low_ref[i] = t[:, 0:LANES].T[0:2]
        high_ref[i] = t[:, length - LANES : length].T[LANES - 2 : LANES]
        return carry

    lax.fori_loop(0, planes, one, 0, unroll=2)


def third_kernel(s_ref, zlo_ref, zhi_ref, out_ref):
    planes, height, length = s_ref.shape

    def one(i, carry):
        gap = jnp.zeros((LANES - 4, height), F32)
        side = jnp.concatenate([zhi_ref[i], gap, zlo_ref[i]], axis=0).T
        t = jnp.concatenate([s_ref[i], side], axis=1)
        out_ref[i] = box(box(t, 1), 1)[:, 0:length]
        return carry

    lax.fori_loop(0, planes, one, 0, unroll=2)


VMEM = pl.BlockSpec(memory_space=pltpu.VMEM)
SMEM = pl.BlockSpec(memory_space=pltpu.SMEM)


def on_device(displacement, density, stiffness):
    planes, height, length = density.shape
    sizes = tuple(lax.axis_size(a) for a in AXES)
    devices = sizes[0] * sizes[1] * sizes[2]
    extents = tuple(n * s for n, s in zip(density.shape, sizes))
    where = jnp.stack([lax.axis_index(a) for a in AXES]).astype(jnp.int32)

    xh = shift_from(displacement[:, :1], "gx", 1)
    yrow = jnp.concatenate([displacement[:, :, 0], xh[:, :, 0]], axis=1)
    yh = shift_from(yrow, "gy", 1)
    zcol = jnp.concatenate([displacement[..., 0], xh[..., 0]], axis=1)
    zcol = jnp.concatenate([zcol, yh[..., :1]], axis=2)
    zh = shift_from(zcol.transpose(1, 0, 2), "gz", 1)
    gap = LANES - height
    zh = jnp.concatenate(
        [
            jnp.pad(zh[..., :height], ((0, 0), (0, 1), (0, gap))),
            jnp.pad(zh[..., 1:], ((0, 0), (0, 1), (0, gap))),
        ],
        axis=1,
    )

    def shape(*dims):
        return jax.ShapeDtypeStruct(dims, F32)

    weighted, low, high, sums = pl.pallas_call(
        functools.partial(energy_kernel, extents=extents),
        in_specs=[SMEM] + [VMEM] * 6,
        out_specs=[VMEM] * 4,
        out_shape=[
            shape(planes, height, length),
            shape(2, height, length),
            shape(2, height, length),
            shape(devices, 1, LANES),
        ],
        scratch_shapes=[
            pltpu.VMEM((2, 12, height, length), F32),
            pltpu.VMEM((48 * ROWS, 24 * ROWS), BF16),
            pltpu.VMEM((height, length), F32),
        ],
        name="energy",
    )(where, displacement, xh, yh, zh, density, stiffness)

    xlo = shift_from(high, "gx", -1)
    xhi = shift_from(low, "gx", 1)
    gathered = lax.all_to_all(sums, AXES, 0, 0, tiled=True)
    totals = jnp.sum(gathered, axis=(0, 1))

    rows = 1 if sizes[1] == 2 else 2
    smooth, *parts = pl.pallas_call(
        first_kernel,
        in_specs=[SMEM] + [VMEM] * 3,
        out_specs=[VMEM] * (1 + rows),
        out_shape=[shape(planes, height, length)] + [shape(planes, 2, length)] * rows,
        name="along_x",
    )(where, weighted, xlo, xhi)
    if rows == 1:
        parts = [lax.ppermute(parts[0], "gy", [(0, 1), (1, 0)])]
    else:
        parts = [shift_from(parts[1], "gy", -1), shift_from(parts[0], "gy", 1)]
    smooth, low, high = pl.pallas_call(
        second_kernel,
        in_specs=[SMEM] + [VMEM] * (1 + rows),
        out_specs=[VMEM] * 3,
        out_shape=[shape(planes, height, length)] + [shape(planes, 2, height)] * 2,
        name="along_y",
    )(where, smooth, *parts)
    zlo = shift_from(high, "gz", -1)
    zhi = shift_from(low, "gz", 1)
    filtered = pl.pallas_call(
        third_kernel,
        in_specs=[VMEM] * 3,
        out_specs=VMEM,
        out_shape=shape(planes, height, length),
        name="along_z",
    )(smooth, zlo, zhi)

    cells = float(extents[0] * extents[1] * extents[2])
    return filtered, totals[0] / cells, totals[1] / cells


def solution(mesh):
    return jax.shard_map(
        on_device,
        mesh=mesh,
        in_specs=(P(None, *AXES), P(*AXES), P()),
        out_specs=(P(*AXES), P(), P()),
        check_vma=False,
    )
```

```python
import functools

import jax
import jax.numpy as jnp
from jax import lax
from jax.experimental import pallas as pl
from jax.experimental.pallas import tpu as pltpu
from jax.sharding import PartitionSpec as P


VOID = 0.001
AXES = ("gx", "gy", "gz")
F32 = jnp.float32
BF16 = jnp.bfloat16
LANES = 128
ROWS = 8


def shift_from(block, axis, distance):
    count = lax.axis_size(axis)
    route = [(i + distance, i) for i in range(count) if 0 <= i + distance < count]
    return lax.ppermute(block, axis, route)


def missing(position, extent):
    lost = (
        3.0 * (position == 0).astype(F32)
        + 1.0 * (position == 1).astype(F32)
        + 3.0 * (position == extent - 1).astype(F32)
        + 1.0 * (position == extent - 2).astype(F32)
    )
    return 9.0 - lost


def setup_kernel(where_ref, k_ref, gains, inv_ref, *, extents):
    height, length = inv_ref.shape
    side = 24 * ROWS
    k = k_ref[...]
    k_hi = k.astype(BF16)
    k_lo = (k - k_hi.astype(F32)).astype(BF16)
    r0 = lax.broadcasted_iota(jnp.int32, (side, 24), 0)
    r1 = lax.broadcasted_iota(jnp.int32, (side, 24), 1)
    spread = (r0 // ROWS == r1).astype(F32).astype(BF16)
    d0 = lax.broadcasted_iota(jnp.int32, (side, side), 0)
    d1 = lax.broadcasted_iota(jnp.int32, (side, side), 1)
    same_row = (d0 % ROWS) == (d1 % ROWS)
    for part, kk in enumerate((k_hi, k_lo)):
        tall = jnp.dot(spread, kk, preferred_element_type=F32).astype(BF16)
        full = lax.dot_general(tall, spread, (((1,), (1,)), ((), ())), preferred_element_type=F32)
        gains[part * side : (part + 1) * side, :] = jnp.where(same_row, full, 0.0).astype(BF16)

    row = lax.broadcasted_iota(jnp.int32, (height, length), 0)
    lane = lax.broadcasted_iota(jnp.int32, (height, length), 1)
    second = missing(row + where_ref[1] * height, extents[1])
    third = missing(lane + where_ref[2] * length, extents[2])
    inv_ref[...] = (-3.0 * (1.0 - VOID)) / (second * third)


def prepare(corners, slot, plane_of, row_of, columns):
    height, length = corners.shape[2:]
    last_row = lax.broadcasted_iota(jnp.int32, (height, length), 0) == height - 1
    last_lane = lax.broadcasted_iota(jnp.int32, (height, length), 1) == length - 1
    turned = jnp.concatenate([columns, jnp.zeros((ROWS - 3, LANES), F32)], axis=0).T
    for m in range(3):
        plane = plane_of(m)
        right = jnp.where(last_lane, turned[0:height, m : m + 1], pltpu.roll(plane, length - 1, 1))
        corners[slot, 4 * m + 0] = plane
        corners[slot, 4 * m + 1] = right
        corners[slot, 4 * m + 2] = jnp.where(last_row, row_of(m, 0), pltpu.roll(plane, height - 1, 0))
        corners[slot, 4 * m + 3] = jnp.where(last_row, row_of(m, 1), pltpu.roll(right, height - 1, 0))


def element_plane(corners, slots, gains, inv_ref, first, rho_of, store, sums):
    height, length = inv_ref.shape
    side = 24 * ROWS
    total, amount = sums
    inv_first = 1.0 / first
    for j in range(height // ROWS):
        rows = slice(j * ROWS, (j + 1) * ROWS)
        x = jnp.concatenate(
            [
                corners[slots[a], 4 * m + 2 * b + c, rows, :]
                for m in range(3)
                for a in range(2)
                for b in range(2)
                for c in range(2)
            ],
            axis=0,
        )
        h = x.astype(BF16)
        y = jnp.dot(gains[...], h, preferred_element_type=F32)
        y = y[:side] + y[side:]
        e = ((2.0 * x - h.astype(F32)) * y).reshape(24, ROWS, length).sum(axis=0)
        rho = rho_of(rows)
        square = rho * rho
        store(rows, square * e * (inv_ref[rows, :] * inv_first))
        total = total + (VOID + square * rho * (1.0 - VOID)) * e
        amount = amount + rho
    return total, amount


def main_kernel(
    where_ref, u_ref, yh_ref, zh_ref, rho_ref, gains, inv_ref, w_ref, low_ref, sums_ref, corners,
    *, extent
):
    planes, _, length = rho_ref.shape

    def load(p, slot):
        prepare(
            corners,
            slot,
            lambda m: u_ref[m, p],
            lambda m, c: yh_ref[m, pl.ds(p, 1), c : c + length],
            zh_ref[p],
        )

    load(0, 0)

    def one(i, slot, sums):
        load(i + 1, 1 - slot)
        at = where_ref[0] * planes + i + jnp.zeros((ROWS, length), jnp.int32)

        def store(rows, value):
            w_ref[i, rows, :] = value

        return element_plane(
            corners, (slot, 1 - slot), gains, inv_ref, missing(at, extent),
            lambda rows: rho_ref[i, rows, :], store, sums,
        )

    zero = jnp.zeros((ROWS, length), F32)
    pairs = (planes - 1) // 2
    sums = lax.fori_loop(0, pairs, lambda t, s: one(2 * t + 1, 1, one(2 * t, 0, s)), (zero, zero))
    for i in range(2 * pairs, planes - 1):
        sums = one(i, i % 2, sums)
    sums_ref[0], sums_ref[1] = sums
    low_ref[...] = w_ref[0:2]


def last_kernel(
    where_ref, u_ref, xh_ref, edge_ref, yh_ref, zh_ref, rho_ref, gains, inv_ref, w_ref, part_ref,
    high_ref, sums_ref, corners, *, extent, planes
):
    length = rho_ref.shape[2]
    last = planes - 1
    prepare(
        corners, 0, lambda m: u_ref[m, 0], lambda m, c: yh_ref[m, last : last + 1, c : c + length], zh_ref[last]
    )
    far = (length // LANES + 1) * LANES
    prepare(
        corners, 1, lambda m: xh_ref[m, 0], lambda m, c: edge_ref[m : m + 1, c : c + length],
        edge_ref[:, far : far + LANES],
    )
    at = where_ref[0] * planes + last + jnp.zeros((ROWS, length), jnp.int32)

    def store(rows, value):
        high_ref[1, rows, :] = value

    total, amount = element_plane(
        corners, (0, 1), gains, inv_ref, missing(at, extent), lambda rows: rho_ref[0, rows, :], store,
        (part_ref[0], part_ref[1]),
    )
    high_ref[0] = w_ref[0]
    at = lax.broadcasted_iota(jnp.int32, sums_ref.shape, 2)
    sums_ref[...] = jnp.where(at == 0, jnp.sum(total), jnp.where(at == 1, jnp.sum(amount), 0.0))


def box(v, axis):
    n = v.shape[axis]
    return v + pltpu.roll(v, 1, axis) + pltpu.roll(v, n - 1, axis)


def first_kernel(where_ref, w_ref, own_ref, xlo_ref, xhi_ref, out_ref, *messages):
    planes, height, _ = w_ref.shape

    def emit(i, five):
        a, b, c, d, e = five
        t = (a + e) + 2.0 * (b + d) + 3.0 * c
        out_ref[i] = t
        low, high = t[0:2], t[height - 2 : height]
        if len(messages) == 1:
            messages[0][i] = jnp.where(where_ref[1] == 0, high, low)
        else:
            messages[0][i] = low
            messages[1][i] = high

    def plane(k):
        if k < 0:
            return xlo_ref[2 + k]
        if k == planes - 1:
            return own_ref[1]
        return w_ref[k] if k < planes else xhi_ref[k - planes]

    for i in (0, 1, planes - 3, planes - 2, planes - 1):
        emit(i, [plane(i + d) for d in range(-2, 3)])

    def inner(i, carry):
        emit(i, [w_ref[i + d] for d in range(-2, 3)])
        return carry

    lax.fori_loop(2, planes - 3, inner, 0, unroll=True)


def second_kernel(where_ref, s_ref, *refs):
    planes, height, length = s_ref.shape
    messages, (out_ref, low_ref, high_ref) = refs[:-3], refs[-3:]

    def one(i, carry):
        if len(messages) == 1:
            got = messages[0][i]
            before = jnp.where(where_ref[1] == 1, got, 0.0)
            after = jnp.where(where_ref[1] == 0, got, 0.0)
        else:
            before, after = messages[0][i], messages[1][i]
        gap = jnp.zeros((ROWS - 4, length), F32)
        t = jnp.concatenate([s_ref[i], after, gap, before], axis=0)
        t = box(box(t, 0), 0)[0:height]
        out_ref[i] = t
        low_ref[i] = t[:, 0:LANES].T[0:2]
        high_ref[i] = t[:, length - LANES : length].T[LANES - 2 : LANES]
        return carry

    lax.fori_loop(0, planes, one, 0, unroll=2)


def third_kernel(s_ref, zlo_ref, zhi_ref, out_ref):
    planes, height, length = s_ref.shape

    def one(i, carry):
        gap = jnp.zeros((LANES - 4, height), F32)
        side = jnp.concatenate([zhi_ref[i], gap, zlo_ref[i]], axis=0).T
        t = jnp.concatenate([s_ref[i], side], axis=1)
        out_ref[i] = box(box(t, 1), 1)[:, 0:length]
        return carry

    lax.fori_loop(0, planes, one, 0, unroll=2)


VMEM = pl.BlockSpec(memory_space=pltpu.VMEM)
SMEM = pl.BlockSpec(memory_space=pltpu.SMEM)


def on_device(displacement, density, stiffness):
    planes, height, length = density.shape
    sizes = tuple(lax.axis_size(a) for a in AXES)
    devices = sizes[0] * sizes[1] * sizes[2]
    extents = tuple(n * s for n, s in zip(density.shape, sizes))
    where = jnp.stack([lax.axis_index(a) for a in AXES]).astype(jnp.int32)

    def shape(*dims):
        return jax.ShapeDtypeStruct(dims, F32)

    zcol = jnp.pad(displacement[..., 0].transpose(1, 0, 2), ((0, 0), (0, 0), (0, LANES - height)))
    zh = shift_from(zcol, "gz", 1)
    xh = shift_from(displacement[:, :1], "gx", 1)
    yrow = jnp.concatenate([displacement[:, :, 0], zh[:, :, :1].transpose(1, 0, 2)], axis=2)
    yh = shift_from(yrow, "gy", 1)
    edge = jnp.concatenate(
        [yh[:, 0], jnp.zeros((3, LANES - 1), F32), zh[0]], axis=1
    )
    edge = shift_from(edge, "gx", 1)

    side = 24 * ROWS
    gains, inverse = pl.pallas_call(
        functools.partial(setup_kernel, extents=extents),
        in_specs=[SMEM, VMEM],
        out_specs=[VMEM, VMEM],
        out_shape=[jax.ShapeDtypeStruct((2 * side, side), BF16), shape(height, length)],
        name="setup",
    )(where, stiffness)
    corner_space = pltpu.VMEM((2, 12, height, length), F32)
    weighted, low, part = pl.pallas_call(
        functools.partial(main_kernel, extent=extents[0]),
        in_specs=[SMEM] + [VMEM] * 6,
        out_specs=[VMEM] * 3,
        out_shape=[shape(planes, height, length), shape(2, height, length), shape(2, ROWS, length)],
        scratch_shapes=[corner_space],
        name="energy",
    )(where, displacement, yh, zh, density, gains, inverse)
    xhi = shift_from(low, "gx", 1)

    def whole(array):
        return pl.BlockSpec(array.shape, lambda i: (0,) * array.ndim)

    def plane_of(at):
        return pl.BlockSpec((1, height, length), lambda i: (at, 0, 0))

    high, sums = pl.pallas_call(
        functools.partial(last_kernel, extent=extents[0], planes=planes),
        grid=(1,),
        in_specs=[
            SMEM,
            pl.BlockSpec((3, 1, height, length), lambda i: (0, planes - 1, 0, 0)),
            whole(xh),
            whole(edge),
            whole(yh),
            whole(zh),
            plane_of(planes - 1),
            whole(gains),
            whole(inverse),
            plane_of(planes - 2),
            whole(part),
        ],
        out_specs=[
            pl.BlockSpec((2, height, length), lambda i: (0, 0, 0)),
            pl.BlockSpec((devices, 1, LANES), lambda i: (0, 0, 0)),
        ],
        out_shape=[shape(2, height, length), shape(devices, 1, LANES)],
        scratch_shapes=[corner_space],
        name="energy_last",
    )(where, displacement, xh, edge, yh, zh, density, gains, inverse, weighted, part)

    xlo = shift_from(high, "gx", -1)
    gathered = lax.all_to_all(sums, AXES, 0, 0, tiled=True)
    totals = jnp.sum(gathered, axis=(0, 1))

    rows = 1 if sizes[1] == 2 else 2
    smooth_x = pl.pallas_call(
        first_kernel,
        in_specs=[SMEM] + [VMEM] * 4,
        out_specs=[VMEM] * (1 + rows),
        out_shape=[shape(planes, height, length)] + [shape(planes, 2, length)] * rows,
        name="along_x",
    )
    smooth, *parts = smooth_x(where, weighted, high, xlo, xhi)
    if rows == 1:
        parts = [lax.ppermute(parts[0], "gy", [(0, 1), (1, 0)])]
    else:
        parts = [shift_from(parts[1], "gy", -1), shift_from(parts[0], "gy", 1)]
    smooth, low, high = pl.pallas_call(
        second_kernel,
        in_specs=[SMEM] + [VMEM] * (1 + rows),
        out_specs=[VMEM] * 3,
        out_shape=[shape(planes, height, length)] + [shape(planes, 2, height)] * 2,
        name="along_y",
    )(where, smooth, *parts)
    zlo = shift_from(high, "gz", -1)
    zhi = shift_from(low, "gz", 1)
    filtered = pl.pallas_call(
        third_kernel,
        in_specs=[VMEM] * 3,
        out_specs=VMEM,
        out_shape=shape(planes, height, length),
        name="along_z",
    )(smooth, zlo, zhi)

    cells = float(extents[0] * extents[1] * extents[2])
    return filtered, totals[0] / cells, totals[1] / cells


def solution(mesh):
    return jax.shard_map(
        on_device,
        mesh=mesh,
        in_specs=(P(None, *AXES), P(*AXES), P()),
        out_specs=(P(*AXES), P(), P()),
        check_vma=False,
    )
```

```python
import functools

import jax
import jax.numpy as jnp
from jax import lax
from jax.experimental import pallas as pl
from jax.experimental.pallas import tpu as pltpu
from jax.sharding import PartitionSpec as P


VOID = 0.001
AXES = ("gx", "gy", "gz")
F32 = jnp.float32
BF16 = jnp.bfloat16
LANES = 128
ROWS = 8


def shift_from(block, axis, distance):
    count = lax.axis_size(axis)
    route = [(i + distance, i) for i in range(count) if 0 <= i + distance < count]
    return lax.ppermute(block, axis, route)


def missing(position, extent):
    lost = (
        3.0 * (position == 0).astype(F32)
        + 1.0 * (position == 1).astype(F32)
        + 3.0 * (position == extent - 1).astype(F32)
        + 1.0 * (position == extent - 2).astype(F32)
    )
    return 9.0 - lost


def setup_kernel(where_ref, k_ref, gains, inv_ref, *, extents):
    height, length = inv_ref.shape
    side = 24 * ROWS
    k = k_ref[...]
    k_hi = k.astype(BF16)
    k_lo = (k - k_hi.astype(F32)).astype(BF16)
    r0 = lax.broadcasted_iota(jnp.int32, (side, 24), 0)
    r1 = lax.broadcasted_iota(jnp.int32, (side, 24), 1)
    spread = (r0 // ROWS == r1).astype(F32).astype(BF16)
    d0 = lax.broadcasted_iota(jnp.int32, (side, side), 0)
    d1 = lax.broadcasted_iota(jnp.int32, (side, side), 1)
    same_row = (d0 % ROWS) == (d1 % ROWS)
    for part, kk in enumerate((k_hi, k_lo)):
        tall = jnp.dot(spread, kk, preferred_element_type=F32).astype(BF16)
        full = lax.dot_general(tall, spread, (((1,), (1,)), ((), ())), preferred_element_type=F32)
        gains[part * side : (part + 1) * side, :] = jnp.where(same_row, full, 0.0).astype(BF16)

    row = lax.broadcasted_iota(jnp.int32, (height, length), 0)
    lane = lax.broadcasted_iota(jnp.int32, (height, length), 1)
    second = missing(row + where_ref[1] * height, extents[1])
    third = missing(lane + where_ref[2] * length, extents[2])
    inv_ref[...] = (-3.0 * (1.0 - VOID)) / (second * third)


def prepare(corners, slot, plane_of, row_of, columns):
    height, length = corners.shape[2:]
    last_row = lax.broadcasted_iota(jnp.int32, (height, length), 0) == height - 1
    last_lane = lax.broadcasted_iota(jnp.int32, (height, length), 1) == length - 1
    turned = jnp.concatenate([columns, jnp.zeros((ROWS - 3, LANES), F32)], axis=0).T
    for m in range(3):
        plane = plane_of(m)
        right = jnp.where(last_lane, turned[0:height, m : m + 1], pltpu.roll(plane, length - 1, 1))
        corners[slot, 4 * m + 0] = plane
        corners[slot, 4 * m + 1] = right
        corners[slot, 4 * m + 2] = jnp.where(last_row, row_of(m, 0), pltpu.roll(plane, height - 1, 0))
        corners[slot, 4 * m + 3] = jnp.where(last_row, row_of(m, 1), pltpu.roll(right, height - 1, 0))


def element_plane(corners, slots, gains, inv_ref, first, rho_of, store, sums):
    height, length = inv_ref.shape
    side = 24 * ROWS
    total, amount = sums
    inv_first = 1.0 / first
    for j in range(height // ROWS):
        rows = slice(j * ROWS, (j + 1) * ROWS)
        x = jnp.concatenate(
            [
                corners[slots[a], 4 * m + 2 * b + c, rows, :]
                for m in range(3)
                for a in range(2)
                for b in range(2)
                for c in range(2)
            ],
            axis=0,
        )
        h = x.astype(BF16)
        y = jnp.dot(gains[...], h, preferred_element_type=F32)
        y = y[:side] + y[side:]
        e = ((2.0 * x - h.astype(F32)) * y).reshape(24, ROWS, length).sum(axis=0)
        rho = rho_of(rows)
        square = rho * rho
        store(rows, square * e * (inv_ref[rows, :] * inv_first))
        total = total + (VOID + square * rho * (1.0 - VOID)) * e
        amount = amount + rho
    return total, amount


def main_kernel(
    where_ref, u_ref, yh_ref, zh_ref, rho_ref, gains, inv_ref, w_ref, low_ref, sums_ref, corners,
    *, extent
):
    planes, _, length = rho_ref.shape

    def load(p, slot):
        prepare(
            corners,
            slot,
            lambda m: u_ref[m, p],
            lambda m, c: yh_ref[m, pl.ds(p, 1), c : c + length],
            zh_ref[p],
        )

    load(0, 0)

    def one(i, slot, sums):
        load(i + 1, 1 - slot)
        at = where_ref[0] * planes + i + jnp.zeros((ROWS, length), jnp.int32)

        def store(rows, value):
            w_ref[i, rows, :] = value

        return element_plane(
            corners, (slot, 1 - slot), gains, inv_ref, missing(at, extent),
            lambda rows: rho_ref[i, rows, :], store, sums,
        )

    zero = jnp.zeros((ROWS, length), F32)
    pairs = (planes - 1) // 2
    sums = lax.fori_loop(0, pairs, lambda t, s: one(2 * t + 1, 1, one(2 * t, 0, s)), (zero, zero))
    for i in range(2 * pairs, planes - 1):
        sums = one(i, i % 2, sums)
    sums_ref[0], sums_ref[1] = sums
    low_ref[...] = w_ref[0:2]


def last_kernel(
    where_ref, u_ref, xh_ref, edge_ref, yh_ref, zh_ref, rho_ref, gains, inv_ref, w_ref, part_ref,
    high_ref, sums_ref, corners, *, extent, planes
):
    length = rho_ref.shape[2]
    last = planes - 1
    prepare(
        corners, 0, lambda m: u_ref[m, 0], lambda m, c: yh_ref[m, last : last + 1, c : c + length], zh_ref[last]
    )
    far = (length // LANES + 1) * LANES
    prepare(
        corners, 1, lambda m: xh_ref[m, 0], lambda m, c: edge_ref[m : m + 1, c : c + length],
        edge_ref[:, far : far + LANES],
    )
    at = where_ref[0] * planes + last + jnp.zeros((ROWS, length), jnp.int32)

    def store(rows, value):
        high_ref[1, rows, :] = value

    total, amount = element_plane(
        corners, (0, 1), gains, inv_ref, missing(at, extent), lambda rows: rho_ref[0, rows, :], store,
        (part_ref[0], part_ref[1]),
    )
    high_ref[0] = w_ref[0]
    at = lax.broadcasted_iota(jnp.int32, sums_ref.shape, 2)
    sums_ref[...] = jnp.where(at == 0, jnp.sum(total), jnp.where(at == 1, jnp.sum(amount), 0.0))


def box(v, axis):
    n = v.shape[axis]
    return v + pltpu.roll(v, 1, axis) + pltpu.roll(v, n - 1, axis)


def first_kernel(where_ref, w_ref, own_ref, xlo_ref, xhi_ref, out_ref, *messages):
    planes, height, _ = w_ref.shape

    def emit(i, five):
        a, b, c, d, e = five
        t = (a + e) + 2.0 * (b + d) + 3.0 * c
        out_ref[i] = t
        low, high = t[0:2], t[height - 2 : height]
        if len(messages) == 1:
            messages[0][i] = jnp.where(where_ref[1] == 0, high, low)
        else:
            messages[0][i] = low
            messages[1][i] = high

    def plane(k):
        if k < 0:
            return xlo_ref[2 + k]
        if k == planes - 1:
            return own_ref[1]
        return w_ref[k] if k < planes else xhi_ref[k - planes]

    for i in (0, 1, planes - 3, planes - 2, planes - 1):
        emit(i, [plane(i + d) for d in range(-2, 3)])

    def inner(i, carry):
        emit(i, [w_ref[i + d] for d in range(-2, 3)])
        return carry

    lax.fori_loop(2, planes - 3, inner, 0, unroll=True)


def second_kernel(where_ref, s_ref, *refs):
    planes, height, length = s_ref.shape
    messages, (out_ref, low_ref, high_ref) = refs[:-3], refs[-3:]
    group = LANES // height
    gap = jnp.zeros((ROWS - 4, length), F32)
    for g in range(planes // group):
        done = []
        for i in range(g * group, (g + 1) * group):
            if len(messages) == 1:
                got = messages[0][i]
                before = jnp.where(where_ref[1] == 1, got, 0.0)
                after = jnp.where(where_ref[1] == 0, got, 0.0)
            else:
                before, after = messages[0][i], messages[1][i]
            t = jnp.concatenate([s_ref[i], after, gap, before], axis=0)
            t = box(box(t, 0), 0)[0:height]
            out_ref[i] = t
            done.append(t)
        at = slice(g * LANES, (g + 1) * LANES)
        low_ref[:, at] = jnp.concatenate([t[:, 0:LANES] for t in done], axis=0).T[0:2]
        high_ref[:, at] = jnp.concatenate([t[:, length - LANES :] for t in done], axis=0).T[LANES - 2 :]


def third_kernel(s_ref, zlo_ref, zhi_ref, out_ref):
    planes, height, length = s_ref.shape
    group = LANES // height
    gap = jnp.zeros((LANES - 4, LANES), F32)
    for g in range(planes // group):
        at = slice(g * LANES, (g + 1) * LANES)
        side = jnp.concatenate([zhi_ref[:, at], gap, zlo_ref[:, at]], axis=0).T
        for k in range(group):
            i = g * group + k
            t = jnp.concatenate([s_ref[i], side[k * height : (k + 1) * height]], axis=1)
            out_ref[i] = box(box(t, 1), 1)[:, 0:length]


VMEM = pl.BlockSpec(memory_space=pltpu.VMEM)
SMEM = pl.BlockSpec(memory_space=pltpu.SMEM)


def on_device(displacement, density, stiffness):
    planes, height, length = density.shape
    sizes = tuple(lax.axis_size(a) for a in AXES)
    devices = sizes[0] * sizes[1] * sizes[2]
    extents = tuple(n * s for n, s in zip(density.shape, sizes))
    where = jnp.stack([lax.axis_index(a) for a in AXES]).astype(jnp.int32)

    def shape(*dims):
        return jax.ShapeDtypeStruct(dims, F32)

    zcol = jnp.pad(displacement[..., 0].transpose(1, 0, 2), ((0, 0), (0, 0), (0, LANES - height)))
    zh = shift_from(zcol, "gz", 1)
    xh = shift_from(displacement[:, :1], "gx", 1)
    yrow = jnp.concatenate([displacement[:, :, 0], zh[:, :, :1].transpose(1, 0, 2)], axis=2)
    yh = shift_from(yrow, "gy", 1)
    edge = jnp.concatenate(
        [yh[:, 0], jnp.zeros((3, LANES - 1), F32), zh[0]], axis=1
    )
    edge = shift_from(edge, "gx", 1)

    side = 24 * ROWS
    setup = pl.pallas_call(
        functools.partial(setup_kernel, extents=extents),
        in_specs=[SMEM, VMEM],
        out_specs=[VMEM, VMEM],
        out_shape=[jax.ShapeDtypeStruct((2 * side, side), BF16), shape(height, length)],
        name="setup",
    )
    gains, inverse = setup(where, stiffness)
    corner_space = pltpu.VMEM((2, 12, height, length), F32)
    weighted, low, part = pl.pallas_call(
        functools.partial(main_kernel, extent=extents[0]),
        in_specs=[SMEM] + [VMEM] * 6,
        out_specs=[VMEM] * 3,
        out_shape=[shape(planes, height, length), shape(2, height, length), shape(2, ROWS, length)],
        scratch_shapes=[corner_space],
        name="energy",
    )(where, displacement, yh, zh, density, gains, inverse)
    xhi = shift_from(low, "gx", 1)

    def whole(array):
        return pl.BlockSpec(array.shape, lambda i: (0,) * array.ndim)

    def plane_of(at):
        return pl.BlockSpec((1, height, length), lambda i: (at, 0, 0))

    high, sums = pl.pallas_call(
        functools.partial(last_kernel, extent=extents[0], planes=planes),
        grid=(1,),
        in_specs=[
            SMEM,
            pl.BlockSpec((3, 1, height, length), lambda i: (0, planes - 1, 0, 0)),
            whole(xh),
            whole(edge),
            whole(yh),
            whole(zh),
            plane_of(planes - 1),
            whole(gains),
            whole(inverse),
            plane_of(planes - 2),
            whole(part),
        ],
        out_specs=[
            pl.BlockSpec((2, height, length), lambda i: (0, 0, 0)),
            pl.BlockSpec((devices, 1, LANES), lambda i: (0, 0, 0)),
        ],
        out_shape=[shape(2, height, length), shape(devices, 1, LANES)],
        scratch_shapes=[corner_space],
        name="energy_last",
    )(where, displacement, xh, edge, yh, zh, density, gains, inverse, weighted, part)

    xlo = shift_from(high, "gx", -1)
    gathered = lax.all_to_all(sums, AXES, 0, 0, tiled=True)
    totals = jnp.sum(gathered, axis=(0, 1))

    rows = 1 if sizes[1] == 2 else 2
    smooth_x = pl.pallas_call(
        first_kernel,
        in_specs=[SMEM] + [VMEM] * 4,
        out_specs=[VMEM] * (1 + rows),
        out_shape=[shape(planes, height, length)] + [shape(planes, 2, length)] * rows,
        name="along_x",
    )
    smooth, *parts = smooth_x(where, weighted, high, xlo, xhi)
    if rows == 1:
        parts = [lax.ppermute(parts[0], "gy", [(0, 1), (1, 0)])]
    else:
        parts = [shift_from(parts[1], "gy", -1), shift_from(parts[0], "gy", 1)]
    smooth, low, high = pl.pallas_call(
        second_kernel,
        in_specs=[SMEM] + [VMEM] * (1 + rows),
        out_specs=[VMEM] * 3,
        out_shape=[shape(planes, height, length)] + [shape(2, planes * height)] * 2,
        name="along_y",
    )(where, smooth, *parts)
    zlo = shift_from(high, "gz", -1)
    zhi = shift_from(low, "gz", 1)
    filtered = pl.pallas_call(
        third_kernel,
        in_specs=[VMEM] * 3,
        out_specs=VMEM,
        out_shape=shape(planes, height, length),
        name="along_z",
    )(smooth, zlo, zhi)

    cells = float(extents[0] * extents[1] * extents[2])
    return filtered, totals[0] / cells, totals[1] / cells


def solution(mesh):
    return jax.shard_map(
        on_device,
        mesh=mesh,
        in_specs=(P(None, *AXES), P(*AXES), P()),
        out_specs=(P(*AXES), P(), P()),
        check_vma=False,
    )
```

```python
import functools

import jax
import jax.numpy as jnp
from jax import lax
from jax.experimental import pallas as pl
from jax.experimental.pallas import tpu as pltpu
from jax.sharding import PartitionSpec as P


VOID = 0.001
AXES = ("gx", "gy", "gz")
F32 = jnp.float32
BF16 = jnp.bfloat16
LANES = 128
ROWS = 8


def shift_from(block, axis, distance):
    count = lax.axis_size(axis)
    route = [(i + distance, i) for i in range(count) if 0 <= i + distance < count]
    return lax.ppermute(block, axis, route)


def missing(position, extent):
    lost = (
        3.0 * (position == 0).astype(F32)
        + 1.0 * (position == 1).astype(F32)
        + 3.0 * (position == extent - 1).astype(F32)
        + 1.0 * (position == extent - 2).astype(F32)
    )
    return 9.0 - lost


def setup_kernel(where_ref, k_ref, gains, inv_ref, *, extents):
    height, length = inv_ref.shape
    side = 24 * ROWS
    k = k_ref[...]
    k_hi = k.astype(BF16)
    k_lo = (k - k_hi.astype(F32)).astype(BF16)
    r0 = lax.broadcasted_iota(jnp.int32, (side, 24), 0)
    r1 = lax.broadcasted_iota(jnp.int32, (side, 24), 1)
    spread = (r0 // ROWS == r1).astype(F32).astype(BF16)
    d0 = lax.broadcasted_iota(jnp.int32, (side, side), 0)
    d1 = lax.broadcasted_iota(jnp.int32, (side, side), 1)
    same_row = (d0 % ROWS) == (d1 % ROWS)
    for part, kk in enumerate((k_hi, k_lo)):
        tall = jnp.dot(spread, kk, preferred_element_type=F32).astype(BF16)
        full = lax.dot_general(tall, spread, (((1,), (1,)), ((), ())), preferred_element_type=F32)
        gains[part * side : (part + 1) * side, :] = jnp.where(same_row, full, 0.0).astype(BF16)

    row = lax.broadcasted_iota(jnp.int32, (height, length), 0)
    lane = lax.broadcasted_iota(jnp.int32, (height, length), 1)
    second = missing(row + where_ref[1] * height, extents[1])
    third = missing(lane + where_ref[2] * length, extents[2])
    inv_ref[...] = (-3.0 * (1.0 - VOID)) / (second * third)


def prepare(corners, slot, plane_of, row_of, columns):
    height, length = corners.shape[2:]
    last_row = lax.broadcasted_iota(jnp.int32, (height, length), 0) == height - 1
    last_lane = lax.broadcasted_iota(jnp.int32, (height, length), 1) == length - 1
    turned = jnp.concatenate([columns, jnp.zeros((ROWS - 3, LANES), F32)], axis=0).T
    for m in range(3):
        plane = plane_of(m)
        right = jnp.where(last_lane, turned[0:height, m : m + 1], pltpu.roll(plane, length - 1, 1))
        corners[slot, 4 * m + 0] = plane
        corners[slot, 4 * m + 1] = right
        corners[slot, 4 * m + 2] = jnp.where(last_row, row_of(m, 0), pltpu.roll(plane, height - 1, 0))
        corners[slot, 4 * m + 3] = jnp.where(last_row, row_of(m, 1), pltpu.roll(right, height - 1, 0))


def element_plane(corners, slots, gains, inv_ref, first, rho_of, store, sums):
    height, length = inv_ref.shape
    side = 24 * ROWS
    total, amount = sums
    inv_first = 1.0 / first
    for j in range(height // ROWS):
        rows = slice(j * ROWS, (j + 1) * ROWS)
        x = jnp.concatenate(
            [
                corners[slots[a], 4 * m + 2 * b + c, rows, :]
                for m in range(3)
                for a in range(2)
                for b in range(2)
                for c in range(2)
            ],
            axis=0,
        )
        h = x.astype(BF16)
        y = jnp.dot(gains[...], h, preferred_element_type=F32)
        y = y[:side] + y[side:]
        e = ((2.0 * x - h.astype(F32)) * y).reshape(24, ROWS, length).sum(axis=0)
        rho = rho_of(rows)
        square = rho * rho
        store(rows, square * e * (inv_ref[rows, :] * inv_first))
        total = total + (VOID + square * rho * (1.0 - VOID)) * e
        amount = amount + rho
    return total, amount


def main_kernel(
    where_ref, u_ref, yh_ref, zh_ref, rho_ref, gains, inv_ref, w_ref, low_ref, sums_ref, corners,
    nodes, arrived, *, extent
):
    planes, _, length = rho_ref.shape

    def fetch(p):
        return pltpu.make_async_copy(u_ref.at[:, p], nodes.at[:, p], arrived.at[p])

    for p in range(planes):
        fetch(p).start()

    def load(p, slot):
        fetch(p).wait()
        prepare(
            corners,
            slot,
            lambda m: nodes[m, p],
            lambda m, c: yh_ref[m, pl.ds(p, 1), c : c + length],
            zh_ref[p],
        )

    load(0, 0)

    def one(i, slot, sums):
        load(i + 1, 1 - slot)
        at = where_ref[0] * planes + i + jnp.zeros((ROWS, length), jnp.int32)

        def store(rows, value):
            w_ref[i, rows, :] = value

        return element_plane(
            corners, (slot, 1 - slot), gains, inv_ref, missing(at, extent),
            lambda rows: rho_ref[i, rows, :], store, sums,
        )

    zero = jnp.zeros((ROWS, length), F32)
    pairs = (planes - 1) // 2
    sums = lax.fori_loop(0, pairs, lambda t, s: one(2 * t + 1, 1, one(2 * t, 0, s)), (zero, zero))
    for i in range(2 * pairs, planes - 1):
        sums = one(i, i % 2, sums)
    sums_ref[0], sums_ref[1] = sums
    low_ref[...] = w_ref[0:2]


def last_kernel(
    where_ref, u_ref, xh_ref, edge_ref, yh_ref, zh_ref, rho_ref, gains, inv_ref, w_ref, part_ref,
    high_ref, sums_ref, corners, *, extent, planes
):
    length = rho_ref.shape[2]
    last = planes - 1
    prepare(
        corners, 0, lambda m: u_ref[m, 0], lambda m, c: yh_ref[m, last : last + 1, c : c + length], zh_ref[last]
    )
    far = (length // LANES + 1) * LANES
    prepare(
        corners, 1, lambda m: xh_ref[m, 0], lambda m, c: edge_ref[m : m + 1, c : c + length],
        edge_ref[:, far : far + LANES],
    )
    at = where_ref[0] * planes + last + jnp.zeros((ROWS, length), jnp.int32)

    def store(rows, value):
        high_ref[1, rows, :] = value

    total, amount = element_plane(
        corners, (0, 1), gains, inv_ref, missing(at, extent), lambda rows: rho_ref[0, rows, :], store,
        (part_ref[0], part_ref[1]),
    )
    high_ref[0] = w_ref[0]
    at = lax.broadcasted_iota(jnp.int32, sums_ref.shape, 2)
    sums_ref[...] = jnp.where(at == 0, jnp.sum(total), jnp.where(at == 1, jnp.sum(amount), 0.0))


def box(v, axis):
    n = v.shape[axis]
    return v + pltpu.roll(v, 1, axis) + pltpu.roll(v, n - 1, axis)


def first_kernel(where_ref, w_ref, own_ref, xlo_ref, xhi_ref, out_ref, *messages):
    planes, height, _ = w_ref.shape

    def emit(i, five):
        a, b, c, d, e = five
        t = (a + e) + 2.0 * (b + d) + 3.0 * c
        out_ref[i] = t
        low, high = t[0:2], t[height - 2 : height]
        if len(messages) == 1:
            messages[0][i] = jnp.where(where_ref[1] == 0, high, low)
        else:
            messages[0][i] = low
            messages[1][i] = high

    def plane(k):
        if k < 0:
            return xlo_ref[2 + k]
        if k == planes - 1:
            return own_ref[1]
        return w_ref[k] if k < planes else xhi_ref[k - planes]

    for i in (0, 1, planes - 3, planes - 2, planes - 1):
        emit(i, [plane(i + d) for d in range(-2, 3)])

    def inner(i, carry):
        emit(i, [w_ref[i + d] for d in range(-2, 3)])
        return carry

    lax.fori_loop(2, planes - 3, inner, 0, unroll=True)


def second_kernel(where_ref, s_ref, *refs):
    planes, height, length = s_ref.shape
    messages, (out_ref, low_ref, high_ref) = refs[:-3], refs[-3:]
    group = LANES // height
    gap = jnp.zeros((ROWS - 4, length), F32)
    for g in range(planes // group):
        done = []
        for i in range(g * group, (g + 1) * group):
            if len(messages) == 1:
                got = messages[0][i]
                before = jnp.where(where_ref[1] == 1, got, 0.0)
                after = jnp.where(where_ref[1] == 0, got, 0.0)
            else:
                before, after = messages[0][i], messages[1][i]
            t = jnp.concatenate([s_ref[i], after, gap, before], axis=0)
            t = box(box(t, 0), 0)[0:height]
            out_ref[i] = t
            done.append(t)
        at = slice(g * LANES, (g + 1) * LANES)
        low_ref[:, at] = jnp.concatenate([t[:, 0:LANES] for t in done], axis=0).T[0:2]
        high_ref[:, at] = jnp.concatenate([t[:, length - LANES :] for t in done], axis=0).T[LANES - 2 :]


def third_kernel(s_ref, zlo_ref, zhi_ref, out_ref):
    planes, height, length = s_ref.shape
    group = LANES // height
    gap = jnp.zeros((LANES - 4, LANES), F32)
    for g in range(planes // group):
        at = slice(g * LANES, (g + 1) * LANES)
        side = jnp.concatenate([zhi_ref[:, at], gap, zlo_ref[:, at]], axis=0).T
        for k in range(group):
            i = g * group + k
            t = jnp.concatenate([s_ref[i], side[k * height : (k + 1) * height]], axis=1)
            out_ref[i] = box(box(t, 1), 1)[:, 0:length]


VMEM = pl.BlockSpec(memory_space=pltpu.VMEM)
SMEM = pl.BlockSpec(memory_space=pltpu.SMEM)


def on_device(displacement, density, stiffness):
    planes, height, length = density.shape
    sizes = tuple(lax.axis_size(a) for a in AXES)
    devices = sizes[0] * sizes[1] * sizes[2]
    extents = tuple(n * s for n, s in zip(density.shape, sizes))
    where = jnp.stack([lax.axis_index(a) for a in AXES]).astype(jnp.int32)

    def shape(*dims):
        return jax.ShapeDtypeStruct(dims, F32)

    zcol = jnp.pad(displacement[..., 0].transpose(1, 0, 2), ((0, 0), (0, 0), (0, LANES - height)))
    zh = shift_from(zcol, "gz", 1)
    xh = shift_from(displacement[:, :1], "gx", 1)
    yrow = jnp.concatenate([displacement[:, :, 0], zh[:, :, :1].transpose(1, 0, 2)], axis=2)
    yh = shift_from(yrow, "gy", 1)
    edge = jnp.concatenate(
        [yh[:, 0], jnp.zeros((3, LANES - 1), F32), zh[0]], axis=1
    )
    edge = shift_from(edge, "gx", 1)

    side = 24 * ROWS
    setup = pl.pallas_call(
        functools.partial(setup_kernel, extents=extents),
        in_specs=[SMEM, VMEM],
        out_specs=[VMEM, VMEM],
        out_shape=[jax.ShapeDtypeStruct((2 * side, side), BF16), shape(height, length)],
        name="setup",
    )
    gains, inverse = setup(where, stiffness)
    corner_space = pltpu.VMEM((2, 12, height, length), F32)
    weighted, low, part = pl.pallas_call(
        functools.partial(main_kernel, extent=extents[0]),
        in_specs=[SMEM, pl.BlockSpec(memory_space=pl.ANY)] + [VMEM] * 5,
        out_specs=[VMEM] * 3,
        out_shape=[shape(planes, height, length), shape(2, height, length), shape(2, ROWS, length)],
        scratch_shapes=[
            corner_space,
            pltpu.VMEM((3, planes, height, length), F32),
            pltpu.SemaphoreType.DMA((planes,)),
        ],
        name="energy",
    )(where, displacement, yh, zh, density, gains, inverse)
    xhi = shift_from(low, "gx", 1)

    def whole(array):
        return pl.BlockSpec(array.shape, lambda i: (0,) * array.ndim)

    def plane_of(at):
        return pl.BlockSpec((1, height, length), lambda i: (at, 0, 0))

    high, sums = pl.pallas_call(
        functools.partial(last_kernel, extent=extents[0], planes=planes),
        grid=(1,),
        in_specs=[
            SMEM,
            pl.BlockSpec((3, 1, height, length), lambda i: (0, planes - 1, 0, 0)),
            whole(xh),
            whole(edge),
            whole(yh),
            whole(zh),
            plane_of(planes - 1),
            whole(gains),
            whole(inverse),
            plane_of(planes - 2),
            whole(part),
        ],
        out_specs=[
            pl.BlockSpec((2, height, length), lambda i: (0, 0, 0)),
            pl.BlockSpec((devices, 1, LANES), lambda i: (0, 0, 0)),
        ],
        out_shape=[shape(2, height, length), shape(devices, 1, LANES)],
        scratch_shapes=[corner_space],
        name="energy_last",
    )(where, displacement, xh, edge, yh, zh, density, gains, inverse, weighted, part)

    xlo = shift_from(high, "gx", -1)
    gathered = lax.all_to_all(sums, AXES, 0, 0, tiled=True)
    totals = jnp.sum(gathered, axis=(0, 1))

    rows = 1 if sizes[1] == 2 else 2
    smooth_x = pl.pallas_call(
        first_kernel,
        in_specs=[SMEM] + [VMEM] * 4,
        out_specs=[VMEM] * (1 + rows),
        out_shape=[shape(planes, height, length)] + [shape(planes, 2, length)] * rows,
        name="along_x",
    )
    smooth, *parts = smooth_x(where, weighted, high, xlo, xhi)
    if rows == 1:
        parts = [lax.ppermute(parts[0], "gy", [(0, 1), (1, 0)])]
    else:
        parts = [shift_from(parts[1], "gy", -1), shift_from(parts[0], "gy", 1)]
    smooth, low, high = pl.pallas_call(
        second_kernel,
        in_specs=[SMEM] + [VMEM] * (1 + rows),
        out_specs=[VMEM] * 3,
        out_shape=[shape(planes, height, length)] + [shape(2, planes * height)] * 2,
        name="along_y",
    )(where, smooth, *parts)
    zlo = shift_from(high, "gz", -1)
    zhi = shift_from(low, "gz", 1)
    filtered = pl.pallas_call(
        third_kernel,
        in_specs=[VMEM] * 3,
        out_specs=VMEM,
        out_shape=shape(planes, height, length),
        name="along_z",
    )(smooth, zlo, zhi)

    cells = float(extents[0] * extents[1] * extents[2])
    return filtered, totals[0] / cells, totals[1] / cells


def solution(mesh):
    return jax.shard_map(
        on_device,
        mesh=mesh,
        in_specs=(P(None, *AXES), P(*AXES), P()),
        out_specs=(P(*AXES), P(), P()),
        check_vma=False,
    )
```
